128 devices in a mesh: row: 8 (over z, y_hi), col: 16 (over y_lo, x, core).
Axes of the slice: x: 4, y: 4 (y_hi: 2, y_lo: 2; y = y_hi * 2 + y_lo), z: 4, core: 2. Of those that a mesh axis runs over, the one named last changes fastest.
Arguments:
- operator: bfloat16 [32768, 32768], P('row', 'col'), may hold values from -6 to 6
- right_test: bfloat16 [32768, 256], P('col'), may hold values from -0.03125 to 0.03125
- left_test: bfloat16 [32768, 384], P('row'), may hold values from -0.03125 to 0.03125
Outputs:
- left_factor: bfloat16 [32768, 256], P(('row', 'col'))
- right_factor: bfloat16 [32768, 256], P('col')
The draws below stay inside these ranges and needn't reach their ends.
All inputs are finite; a program needn't handle non-finite values.
Results may differ from the reference program's by a relative error of at most 0.0015.
Values may be sent and summed in bfloat16 or wider, within the bound.
A program may use at most 128 MiB of HBM per device.

```python
import jax
import jax.numpy as jnp
from jax import lax

N = 32768
R1 = 256
R2 = 384


def spiked(values, rng, source, target, blocks, factor):
    owner, partner = [(jnp.arange(values.shape[axis_at]) // (values.shape[axis_at] // blocks)).reshape([-1 if axis == axis_at else 1 for axis in range(values.ndim)]) for axis_at in (source, target)]
    chosen = jax.random.permutation(rng, blocks)[partner]
    strong = (owner == chosen) | (owner == (partner + blocks // 2) % blocks)
    return jnp.where(strong, factor * values, values)


def block_levels(own_key, extent, shards, low, largest):
    factor_of = 1.0
    for position, blocks in shards:
        draws = jax.random.uniform(jax.random.fold_in(jax.random.fold_in(own_key, 6), position), (blocks,), jnp.float32, low / len(shards), largest / len(shards))
        factor_of = factor_of * jnp.repeat(jnp.exp(draws), extent[position] // blocks).reshape((-1,) + (1,) * (len(extent) - 1 - position))
    return factor_of


def centred(stream_key, shape, width, reach, cuts=(), kind=jnp.bfloat16):
    level = block_levels(stream_key, shape, cuts, -0.22, 0.18) if cuts else 1.0
    drawn = jax.random.normal(stream_key, shape, jnp.float32) * width * level
    return jnp.minimum(jnp.maximum(drawn, -reach), reach).astype(kind)


def bell_draw_with(stream_key, extent, deviation, reach, cuts, heavy, held_as=jnp.bfloat16):
    result = deviation * jax.random.normal(stream_key, extent, jnp.float32)
    if cuts:
        result = result * block_levels(stream_key, extent, cuts, -0.22, 0.18)
    return jnp.clip(spiked(result, jax.random.fold_in(stream_key, 3), *heavy), -reach, reach).astype(held_as)


def setup_inputs(seed: int = 0) -> dict:
    seeds = jax.random.split(jax.random.key(seed), 4)
    operator = bell_draw_with(seeds[0], (N, N), 1.0, 6.0, ((0, 8), (1, 16)), (1, 0, 16, 2.0))
    right_test = centred(seeds[1], (N, R1), N ** -0.5, 0.03125, ((0, 16),))
    left_test = centred(seeds[2], (N, R2), N ** -0.5, 0.03125, ((0, 8),))
    return {"operator": operator, "right_test": right_test, "left_test": left_test}


def reference(operator, right_test, left_test):
    left_sketch = jnp.dot(operator.astype(jnp.float32), right_test.astype(jnp.float32), preferred_element_type=jnp.float32)
    right_sketch = lax.dot_general(operator.astype(jnp.float32), left_test.astype(jnp.float32), (((0,), (0,)), ((), ())), preferred_element_type=jnp.float32)
    core_matrix = lax.dot_general(left_test.astype(jnp.float32), left_sketch, (((0,), (0,)), ((), ())), precision=lax.Precision.HIGHEST)
    gram_plain = jnp.dot(core_matrix.T, core_matrix, precision=lax.Precision.HIGHEST)
    shift_size = 0.001 * jnp.trace(gram_plain) / R1
    gram_matrix = gram_plain + shift_size * jnp.eye(R1, dtype=jnp.float32)
    lower_factor = jnp.linalg.cholesky(gram_matrix)
    solve_map = jax.scipy.linalg.cho_solve((lower_factor, True), core_matrix.T)
    right_factor = jnp.dot(right_sketch, solve_map.T, precision=lax.Precision.HIGHEST).astype(jnp.bfloat16)
    return (left_sketch.astype(jnp.bfloat16), right_factor)
```

```python
import jax
import jax.numpy as jnp
from jax import lax
from jax.experimental import pallas as pl
from jax.experimental.pallas import tpu as pltpu
from jax.sharding import PartitionSpec as P

MESH = pl.DeviceIdType.MESH
F32 = jnp.float32
BF16 = jnp.bfloat16
HIGHEST = lax.Precision.HIGHEST
SCALE_ROWS = 16
TOP = 2.0**15


def dot(a, b, dims=((1,), (0,)), precision=None):
    return lax.dot_general(a, b, (dims, ((), ())), precision=precision, preferred_element_type=F32)


def largest(value):
    return jnp.maximum(jnp.max(jnp.abs(value), axis=(0, 1), keepdims=True), 1e-30)


def store_coded(ref, value):
    rows, columns = value.shape
    scale = jnp.broadcast_to(largest(value) * 1.01, (SCALE_ROWS, columns)).astype(BF16)
    ref[pl.ds(rows, SCALE_ROWS), :] = scale
    t = value * (TOP / scale.astype(F32)[0:1, :])
    t2 = t * t
    t4 = t2 * t2
    t8 = t4 * t4
    ref[pl.ds(0, rows), :] = jnp.where(t < 0, -t8, t8).astype(BF16)


def load_coded(ref, rows):
    scale = ref[pl.ds(rows, SCALE_ROWS), :].astype(F32)[0:1, :] * (1.0 / TOP)
    y = ref[pl.ds(0, rows), :].astype(F32)
    r = jnp.sqrt(jnp.sqrt(jnp.sqrt(jnp.abs(y)))) * scale
    return jnp.where(y < 0, -r, r)


def inverse_128(a):
    n = a.shape[0]
    sub = lax.broadcasted_iota(jnp.int32, (8, n), 0)
    lane8 = lax.broadcasted_iota(jnp.int32, (8, n), 1)
    lane = lax.broadcasted_iota(jnp.int32, (n, n), 1)
    for k0 in range(0, n, 8):
        p = a[k0 : k0 + 8, :]
        c = [jnp.broadcast_to(p[:, k0 + j : k0 + j + 1], (8, n)) for j in range(8)]
        for k in range(8):
            r = 1.0 / c[k][k : k + 1, :]
            ck = c[k]
            new = []
            for j in range(8):
                if j == k:
                    new.append(jnp.where(sub == k, r, -ck * r))
                else:
                    pj = c[j][k : k + 1, :] * r
                    new.append(jnp.where(sub == k, pj, c[j] - ck * pj))
            c = new
        inside8 = (lane8 >= k0) & (lane8 < k0 + 8)
        pivot = jnp.where(inside8, jnp.where(lane8 == sub + k0, 1.0, 0.0), p)
        x = c[0] * pivot[0:1, :]
        for j in range(1, 8):
            x = x + c[j] * pivot[j : j + 1, :]
        inside = (lane >= k0) & (lane < k0 + 8)
        rest = jnp.where(inside, 0.0, a)
        for j in range(8):
            rest = rest - a[:, k0 + j : k0 + j + 1] * x[j : j + 1, :]
        pieces = [rest[:k0]] * (k0 > 0) + [x] + [rest[k0 + 8 :]] * (k0 + 8 < n)
        a = jnp.concatenate(pieces, axis=0)
    return a


def inverse_256(g):
    h = g.shape[0] // 2
    a, b, d = g[:h, :h], g[:h, h:], g[h:, h:]
    ai = inverse_128(a)
    y = dot(ai, b, precision=HIGHEST)
    si = inverse_128(d - dot(b, y, ((0,), (0,)), HIGHEST))
    t = dot(y, si, precision=HIGHEST)
    top = ai + dot(t, y, ((1,), (1,)), HIGHEST)
    return jnp.concatenate(
        [jnp.concatenate([top, -t], axis=1), jnp.concatenate([-t.T, si], axis=1)], axis=0
    )


def kernel(
    a_hbm, r_hbm, l_hbm, left_out, right_out,
    a_v, r_v, l_v, lt_v, acc, lacc,
    cbuf, cd, h1, cx, h2, cy, h3, cz, g0,
    rsend, rz, rsum, ysend, ry, ag,
    ld, lsend, lr, w_hi, w_lo,
    in_sem, ss, rs,
):
    m, n = a_hbm.shape
    r1 = r_hbm.shape[1]
    r2 = l_hbm.shape[1]
    row, col = lax.axis_index("row"), lax.axis_index("col")
    z, yh = row // 2, row % 2
    yl, x, core = col // 8, (col // 2) % 4, col % 2
    y = yh * 2 + yl
    share = 256

    def dev(zz, yy, xx, cc):
        return (zz * 2 + yy // 2, (yy % 2) * 8 + xx * 2 + cc)

    chunk = m // 4
    loads = []
    for i in range(4):
        part = pl.ds(i * chunk, chunk)
        loads.append(pltpu.make_async_copy(l_hbm.at[part], l_v.at[part], in_sem.at[2 * i]))
        loads.append(pltpu.make_async_copy(a_hbm.at[part], a_v.at[part], in_sem.at[2 * i + 1]))
    loads.append(pltpu.make_async_copy(r_hbm, r_v, in_sem.at[8]))
    for load in loads:
        load.start()

    partner = dev(z, y, x, 1 - core)
    z_peers = [dev((z + k) % 4, y, x, core) for k in (1, 2, 3)]
    y_peers = [dev(z, (y + k) % 4, x, core) for k in (1, 2, 3)]
    x_peers = [dev(z, y, (x + k) % 4, core) for k in (1, 2, 3)]
    xy_peers = [dev(z, yh * 2 + 1 - yl, (x + k) % 4, core) for k in (1, 2, 3)]
    flip_yl = dev(z, yh * 2 + 1 - yl, x, core)
    flip_yh = dev(z, (1 - yh) * 2 + yl, x, core)
    barrier = pltpu.get_barrier_semaphore()
    for peer in [partner] + z_peers + y_peers + x_peers + xy_peers:
        pl.semaphore_signal(barrier, inc=1, device_id=peer, device_id_type=MESH)

    count = [0]
    started = []

    def push(src, dst, peer):
        i = count[0]
        count[0] += 1
        copy = pltpu.make_async_remote_copy(
            src_ref=src, dst_ref=dst, send_sem=ss.at[i], recv_sem=rs.at[i],
            device_id=peer, device_id_type=MESH,
        )
        copy.start()
        started.append(copy)
        return copy

    acc[...] = jnp.zeros_like(acc)

    for i in range(4):
        loads[2 * i].wait()
        lt_v[...] = l_v[pl.ds(i * chunk, chunk), :].T
        loads[2 * i + 1].wait()

        @pl.loop(0, n // 256)
        def _(t):
            here = pl.ds(pl.multiple_of(t * 256, 256), 256)
            acc[:, here] += dot(lt_v[...], a_v[pl.ds(i * chunk, chunk), here])

    loads[8].wait()
    core_part = jnp.zeros((r2, r1), F32)
    cbuf[...] = jnp.zeros_like(cbuf)

    @pl.loop(0, n // 512)
    def _(t):
        here = pl.ds(pl.multiple_of(t * 512, 512), 512)
        v = acc[:, here]
        hi = v.astype(BF16)
        v = v - hi.astype(F32)
        mid = v.astype(BF16)
        lo = (v - mid.astype(F32)).astype(BF16)
        rt = r_v[here, :]
        part = dot(hi, rt) + (dot(mid, rt) + dot(lo, rt))
        cbuf[pl.ds(0, r2), :] += part[:, :128]
        cbuf[pl.ds(r2, r2), :] += part[:, 128:]

    pl.semaphore_wait(barrier, 13)

    half = pl.multiple_of((1 - core) * r2, 8)
    c_d = push(cbuf.at[pl.ds(half, r2)], cd, partner)

    @pl.loop(0, 8)
    def _(q):
        here = pl.ds(pl.multiple_of(q * share, share), share)
        store_coded(rsend.at[q], acc[:, here])

    right_z = [
        push(rsend.at[pl.ds(((z + k) % 4) * 2, 2)], rz.at[k - 1], z_peers[k - 1]) for k in (1, 2, 3)
    ]

    c_d.wait_recv()
    h1[...] = cbuf[pl.ds(pl.multiple_of(core * r2, 8), r2), :] + cd[...]
    n1 = r2 // 4
    c_x = [
        push(h1.at[pl.ds(pl.multiple_of(((x + k) % 4) * n1, 8), n1)], cx.at[k - 1], x_peers[k - 1])
        for k in (1, 2, 3)
    ]

    @pl.loop(0, 8)
    def _(q):
        rows = pl.ds(pl.multiple_of(q * 512, 512), 512)
        part = dot(a_v[rows, :], r_v[...])
        lacc[q, 0] = part[:256]
        lacc[q, 1] = part[256:]

    left_d = push(lacc.at[:, 1 - core], ld, partner)

    for copy in c_x:
        copy.wait_recv()
    h2[...] = h1[pl.ds(pl.multiple_of(x * n1, 8), n1), :] + (cx[0] + cx[1] + cx[2])
    n2 = n1 // 4
    c_y = [
        push(h2.at[pl.ds(pl.multiple_of(((y + k) % 4) * n2, 8), n2)], cy.at[k - 1], y_peers[k - 1])
        for k in (1, 2, 3)
    ]
    for copy in c_y:
        copy.wait_recv()
    h3[...] = h2[pl.ds(pl.multiple_of(y * n2, 8), n2), :] + (cy[0] + cy[1] + cy[2])
    cz[z] = h3[...]
    c_z = [push(h3, cz.at[z], z_peers[k - 1]) for k in (1, 2, 3)]

    left_d.wait_recv()
    me_q = yl * 4 + x

    @pl.loop(0, 8)
    def _(q):
        store_coded(lsend.at[q], lacc[q, core] + ld[q])

    for copy in c_z:
        copy.wait_recv()
    base2 = pl.multiple_of(core * r2 + x * n1, 8)
    base3 = pl.multiple_of(core * r2 + x * n1 + y * n2, 8)
    g0[pl.ds(base3, n2), :] = (cz[0] + cz[1]) + (cz[2] + cz[3])
    own = g0.at[pl.ds(base3, n2)]
    g_y = [push(own, own, y_peers[k - 1]) for k in (1, 2, 3)]

    left_flip = push(lsend.at[(1 - yl) * 4 + x], lr.at[0], flip_yl)
    left_x = [push(lsend.at[yl * 4 + (x + k) % 4], lr.at[k], x_peers[k - 1]) for k in (1, 2, 3)]
    left_xy = [
        push(lsend.at[(1 - yl) * 4 + (x + k) % 4], lr.at[k + 3], xy_peers[k - 1]) for k in (1, 2, 3)
    ]

    for copy in g_y:
        copy.wait_recv()
    own = g0.at[pl.ds(base2, n1)]
    g_x = [push(own, own, x_peers[k - 1]) for k in (1, 2, 3)]

    for copy in right_z:
        copy.wait_recv()

    @pl.loop(0, 2)
    def _(h):
        here = pl.ds(pl.multiple_of((z * 2 + h) * share, share), share)
        total = acc[:, here]
        for k in range(3):
            total = total + load_coded(rz.at[k, h], r2)
        rsum[h] = total

    store_coded(ysend, rsum[1 - yh])
    right_y = push(ysend, ry, flip_yh)

    for copy in g_x:
        copy.wait_recv()
    own = g0.at[pl.ds(pl.multiple_of(core * r2, 8), r2)]
    g_d = push(own, own, partner)

    right_y.wait_recv()
    store_coded(ag.at[row], (rsum[yh] + load_coded(ry, r2)).T)
    ag_y = push(ag.at[row], ag.at[row], flip_yh)

    g_d.wait_recv()
    core_all = jnp.concatenate([g0[pl.ds(0, r2), :], g0[pl.ds(r2, r2), :]], axis=1)
    gram = dot(core_all, core_all, ((0,), (0,)), HIGHEST)
    eye = jnp.where(
        lax.broadcasted_iota(jnp.int32, (r1, r1), 0) == lax.broadcasted_iota(jnp.int32, (r1, r1), 1), 1.0, 0.0
    )
    shift = jnp.sum(gram * eye, axis=(0, 1), keepdims=True) * 0.001 / r1
    gram = gram + shift * eye

    ag_y.wait_recv()
    both = ag.at[pl.ds(z * 2, 2)]
    ag_z = [push(both, both, z_peers[k - 1]) for k in (1, 2, 3)]

    w = dot(core_all, inverse_256(gram), precision=HIGHEST)
    w_hi[...] = w.astype(BF16)
    w_lo[...] = (w - w_hi[...].astype(F32)).astype(BF16)

    for copy in [left_flip] + left_x + left_xy:
        copy.wait_recv()
    total = lacc[me_q, core] + ld[me_q]
    for k in range(7):
        total = total + load_coded(lr.at[k], share)
    left_out[...] = total.astype(BF16)

    for copy in ag_z:
        copy.wait_recv()

    @pl.loop(0, 8)
    def _(q):
        b = load_coded(ag.at[q], share)
        hi = b.astype(BF16)
        lo = (b - hi.astype(F32)).astype(BF16)
        v = dot(hi, w_hi[...]) + (dot(hi, w_lo[...]) + dot(lo, w_hi[...]))
        right_out[pl.ds(pl.multiple_of(q * share, share), share), :] = v.astype(BF16)

    for copy in started:
        copy.wait_send()


def body(operator, right_test, left_test):
    m, n = operator.shape
    r1, r2 = right_test.shape[1], left_test.shape[1]
    share = 256
    coded = SCALE_ROWS
    vmem = pltpu.VMEM
    n1, n2 = r2 // 4, r2 // 16
    copies = 40
    return pl.pallas_call(
        kernel,
        out_shape=(
            jax.ShapeDtypeStruct((share, r1), BF16),
            jax.ShapeDtypeStruct((n, r1), BF16),
        ),
        in_specs=[pl.BlockSpec(memory_space=pl.ANY)] * 3,
        out_specs=(pl.BlockSpec(memory_space=pltpu.VMEM),) * 2,
        scratch_shapes=[
            vmem((m, n), BF16), vmem((n, r1), BF16), vmem((m, r2), BF16), vmem((r2, m // 4), BF16),
            vmem((r2, n), F32), vmem((8, 2, share, r1), F32),
            vmem((2 * r2, 128), F32), vmem((r2, 128), F32), vmem((r2, 128), F32),
            vmem((3, n1, 128), F32), vmem((n1, 128), F32), vmem((3, n2, 128), F32),
            vmem((n2, 128), F32), vmem((4, n2, 128), F32), vmem((2 * r2, 128), F32),
            vmem((8, r2 + coded, share), BF16), vmem((3, 2, r2 + coded, share), BF16),
            vmem((2, r2, share), F32), vmem((r2 + coded, share), BF16), vmem((r2 + coded, share), BF16),
            vmem((8, share + coded, r2), BF16),
            vmem((8, share, r1), F32), vmem((8, share + coded, r1), BF16), vmem((7, share + coded, r1), BF16),
            vmem((r2, r1), BF16), vmem((r2, r1), BF16),
            pltpu.SemaphoreType.DMA((9,)), pltpu.SemaphoreType.DMA((copies,)), pltpu.SemaphoreType.DMA((copies,)),
        ],
        compiler_params=pltpu.CompilerParams(
            collective_id=0, has_side_effects=True, vmem_limit_bytes=66_000_000
        ),
    )(operator, right_test, left_test)


def solution(mesh):
    placed = (P("row", "col"), P("col", None), P("row", None))
    return jax.shard_map(
        body,
        mesh=mesh,
        in_specs=placed,
        out_specs=(P(("row", "col"), None), P("col", None)),
        check_vma=False,
    )
```

```python
import jax
import jax.numpy as jnp
from jax import lax
from jax.experimental import pallas as pl
from jax.experimental.pallas import tpu as pltpu
from jax.sharding import PartitionSpec as P

MESH = pl.DeviceIdType.MESH
F32 = jnp.float32
BF16 = jnp.bfloat16
HIGHEST = lax.Precision.HIGHEST
SCALE_ROWS = 16
TOP = 2.0**15


def dot(a, b, dims=((1,), (0,)), precision=None):
    return lax.dot_general(a, b, (dims, ((), ())), precision=precision, preferred_element_type=F32)


def largest(value):
    return jnp.maximum(jnp.max(jnp.abs(value), axis=(0, 1), keepdims=True), 1e-30)


def store_coded(ref, value):
    rows, columns = value.shape
    scale = jnp.broadcast_to(largest(value) * 1.01, (SCALE_ROWS, columns)).astype(BF16)
    ref[pl.ds(rows, SCALE_ROWS), :] = scale
    t = value * (TOP / scale.astype(F32)[0:1, :])
    t2 = t * t
    t4 = t2 * t2
    t8 = t4 * t4
    ref[pl.ds(0, rows), :] = jnp.where(t < 0, -t8, t8).astype(BF16)


def load_coded(ref, rows):
    scale = ref[pl.ds(rows, SCALE_ROWS), :].astype(F32)[0:1, :] * (1.0 / TOP)
    y = ref[pl.ds(0, rows), :].astype(F32)
    r = jnp.sqrt(jnp.sqrt(jnp.sqrt(jnp.abs(y)))) * scale
    return jnp.where(y < 0, -r, r)


def inverse_128(a):
    n = a.shape[0]
    sub = lax.broadcasted_iota(jnp.int32, (8, n), 0)
    lane8 = lax.broadcasted_iota(jnp.int32, (8, n), 1)
    lane = lax.broadcasted_iota(jnp.int32, (n, n), 1)
    for k0 in range(0, n, 8):
        p = a[k0 : k0 + 8, :]
        c = [jnp.broadcast_to(p[:, k0 + j : k0 + j + 1], (8, n)) for j in range(8)]
        for k in range(8):
            r = 1.0 / c[k][k : k + 1, :]
            ck = c[k]
            new = []
            for j in range(8):
                if j == k:
                    new.append(jnp.where(sub == k, r, -ck * r))
                else:
                    pj = c[j][k : k + 1, :] * r
                    new.append(jnp.where(sub == k, pj, c[j] - ck * pj))
            c = new
        inside8 = (lane8 >= k0) & (lane8 < k0 + 8)
        pivot = jnp.where(inside8, jnp.where(lane8 == sub + k0, 1.0, 0.0), p)
        x = c[0] * pivot[0:1, :]
        for j in range(1, 8):
            x = x + c[j] * pivot[j : j + 1, :]
        inside = (lane >= k0) & (lane < k0 + 8)
        rest = jnp.where(inside, 0.0, a)
        for j in range(8):
            rest = rest - a[:, k0 + j : k0 + j + 1] * x[j : j + 1, :]
        pieces = [rest[:k0]] * (k0 > 0) + [x] + [rest[k0 + 8 :]] * (k0 + 8 < n)
        a = jnp.concatenate(pieces, axis=0)
    return a


def inverse_256(g):
    h = g.shape[0] // 2
    a, b, d = g[:h, :h], g[:h, h:], g[h:, h:]
    ai = inverse_128(a)
    y = dot(ai, b, precision=HIGHEST)
    si = inverse_128(d - dot(b, y, ((0,), (0,)), HIGHEST))
    t = dot(y, si, precision=HIGHEST)
    top = ai + dot(t, y, ((1,), (1,)), HIGHEST)
    return jnp.concatenate(
        [jnp.concatenate([top, -t], axis=1), jnp.concatenate([-t.T, si], axis=1)], axis=0
    )


def kernel(
    a_hbm, r_hbm, l_hbm, left_out, right_out,
    a_v, r_v, l_v, lt_v, acc, lacc,
    cbuf, cd, h1, cx, h2, cy, h3, cz, g0,
    rsend, rz, rsum, ysend, ry, ag,
    ld, lsend, lx, lsum, lysend, ly, w_hi, w_lo,
    in_sem, ss, rs,
):
    m, n = a_hbm.shape
    r1 = r_hbm.shape[1]
    r2 = l_hbm.shape[1]
    row, col = lax.axis_index("row"), lax.axis_index("col")
    z, yh = row // 2, row % 2
    yl, x, core = col // 8, (col // 2) % 4, col % 2
    y = yh * 2 + yl
    share = n // 8
    group = 2 * share

    def dev(zz, yy, xx, cc):
        return (zz * 2 + yy // 2, (yy % 2) * 8 + xx * 2 + cc)

    chunk = m // 4
    load_l = []
    for i in range(4):
        part = pl.ds(i * chunk, chunk)
        load_l.append(pltpu.make_async_copy(l_hbm.at[part], l_v.at[part], in_sem.at[i]))
    order = (2, 1, 3, 0)
    columns = [pl.ds(pl.multiple_of(((z + k) % 4) * group, group), group) for k in order]
    load_a = [
        pltpu.make_async_copy(a_hbm.at[:, here], a_v.at[:, here], in_sem.at[4 + i])
        for i, here in enumerate(columns)
    ]
    load_r = pltpu.make_async_copy(r_hbm, r_v, in_sem.at[8])
    for load in load_l + load_a + [load_r]:
        load.start()

    partner = dev(z, y, x, 1 - core)
    z_peers = [dev((z + k) % 4, y, x, core) for k in (1, 2, 3)]
    y_peers = [dev(z, (y + k) % 4, x, core) for k in (1, 2, 3)]
    x_peers = [dev(z, y, (x + k) % 4, core) for k in (1, 2, 3)]
    xy_peers = [dev(z, yh * 2 + 1 - yl, (x + k) % 4, core) for k in (1, 2, 3)]
    flip_yl = dev(z, yh * 2 + 1 - yl, x, core)
    flip_yh = dev(z, (1 - yh) * 2 + yl, x, core)
    barrier = pltpu.get_barrier_semaphore()
    for peer in [partner] + z_peers + y_peers + x_peers + xy_peers:
        pl.semaphore_signal(barrier, inc=1, device_id=peer, device_id_type=MESH)

    count = [0]
    started = []

    def push(src, dst, peer):
        i = count[0]
        count[0] += 1
        copy = pltpu.make_async_remote_copy(
            src_ref=src, dst_ref=dst, send_sem=ss.at[i], recv_sem=rs.at[i],
            device_id=peer, device_id_type=MESH,
        )
        copy.start()
        started.append(copy)
        return copy

    for i in range(4):
        part = pl.ds(i * chunk, chunk)
        load_l[i].wait()
        lt_v[:, part] = l_v[part, :].T

    right_z = [None] * 4

    def code_chunk(i):
        for h in range(2):
            store_coded(rsend.at[i, h], acc[i, :, h * share : (h + 1) * share])

    def send_chunk(i):
        k = order[i]
        right_z[k] = push(rsend.at[i], rz.at[k - 1], z_peers[k - 1])

    for i in range(4):
        load_a[i].wait()
        if i:
            code_chunk(i - 1)
        acc[i] = dot(lt_v[...], a_v[:, columns[i]])
        if i == 0:
            pl.semaphore_wait(barrier, 13)
        else:
            send_chunk(i - 1)

    load_r.wait()
    part = None
    for i in range(4):
        v = acc[i]
        hi = v.astype(BF16)
        v = v - hi.astype(F32)
        mid = v.astype(BF16)
        lo = (v - mid.astype(F32)).astype(BF16)
        rt = r_v[columns[i], :]
        term = dot(hi, rt) + (dot(mid, rt) + dot(lo, rt))
        part = term if part is None else part + term
    cbuf[pl.ds(0, r2), :] = part[:, :128]
    cbuf[pl.ds(r2, r2), :] = part[:, 128:]
    c_d = push(cbuf.at[pl.ds(pl.multiple_of((1 - core) * r2, 8), r2)], cd, partner)

    def left_half(i):
        @pl.loop(0, 2)
        def _(t):
            rows = pl.ds(pl.multiple_of((2 * i + t) * (m // 4), m // 4), m // 4)
            product = dot(a_v[rows, :], r_v[...])
            lacc[pl.ds(4 * i + 2 * t, 2)] = product.reshape(2, 2, m // 16, r1)

        return push(lacc.at[pl.ds(4 * i, 4), 1 - core], ld.at[pl.ds(4 * i, 4)], partner)

    left_x = []

    def left_send(i):
        left_d[i].wait_recv()
        for k in (2, 1, 3):
            q = 4 * i + (x + k) % 4
            store_coded(lsend.at[i, k - 1], lacc[q, core] + ld[q])
            left_x.append(push(lsend.at[i, k - 1], lx.at[i, k - 1], x_peers[k - 1]))

    left_d = [left_half(0)]
    c_d.wait_recv()
    h1[...] = cbuf[pl.ds(pl.multiple_of(core * r2, 8), r2), :] + cd[...]
    n1 = r2 // 4
    c_x = [
        push(h1.at[pl.ds(pl.multiple_of(((x + k) % 4) * n1, 8), n1)], cx.at[k - 1], x_peers[k - 1])
        for k in (1, 2, 3)
    ]
    left_d.append(left_half(1))
    left_send(0)

    for copy in c_x:
        copy.wait_recv()
    h2[...] = h1[pl.ds(pl.multiple_of(x * n1, 8), n1), :] + (cx[0] + cx[1] + cx[2])
    n2 = n1 // 4
    c_y = [
        push(h2.at[pl.ds(pl.multiple_of(((y + k) % 4) * n2, 8), n2)], cy.at[k - 1], y_peers[k - 1])
        for k in (1, 2, 3)
    ]
    left_send(1)

    for copy in c_y:
        copy.wait_recv()
    h3[...] = h2[pl.ds(pl.multiple_of(y * n2, 8), n2), :] + (cy[0] + cy[1] + cy[2])
    cz[z] = h3[...]
    c_z = [push(h3, cz.at[z], z_peers[k - 1]) for k in (1, 2, 3)]

    for copy in right_z[1:]:
        copy.wait_recv()

    def right_total(h):
        here = pl.ds(pl.multiple_of(h * share, share), share)
        total = acc[3, :, here]
        for k in range(3):
            total = total + load_coded(rz.at[k, h], r2)
        return total

    store_coded(ysend, right_total(1 - yh))
    right_y = push(ysend, ry, flip_yh)
    rsum[...] = right_total(yh)

    for copy in c_z:
        copy.wait_recv()
    base2 = pl.multiple_of(core * r2 + x * n1, 8)
    base3 = pl.multiple_of(core * r2 + x * n1 + y * n2, 8)
    g0[pl.ds(base3, n2), :] = (cz[0] + cz[1]) + (cz[2] + cz[3])
    own = g0.at[pl.ds(base3, n2)]
    g_y = [push(own, own, y_peers[k - 1]) for k in (1, 2, 3)]

    for copy in g_y:
        copy.wait_recv()
    own = g0.at[pl.ds(base2, n1)]
    g_x = [push(own, own, x_peers[k - 1]) for k in (1, 2, 3)]

    right_y.wait_recv()
    v = (rsum[...] + load_coded(ry, r2)).T
    half = share // 2
    store_coded(ag.at[row, 1], v[half:])
    store_coded(ag.at[row, 0], v[:half])

    def slot(zz, yyh, which):
        return ag.at[zz * 2 + yyh, which]

    own_a, own_b = slot(z, yh, 0), slot(z, yh, 1)
    b_z = [push(own_b, own_b, z_peers[k - 1]) for k in (1, 2, 3)]
    a_y = push(own_a, own_a, flip_yh)
    b_y = [push(own_b, own_b, flip_yh)]
    a_z = [push(own_a, own_a, z_peers[k - 1]) for k in (1, 2, 3)]

    for copy in g_x:
        copy.wait_recv()
    own = g0.at[pl.ds(pl.multiple_of(core * r2, 8), r2)]
    g_d = push(own, own, partner)

    for copy in left_x:
        copy.wait_recv()

    def left_total(h):
        q = 4 * h + x
        total = lacc[q, core] + ld[q]
        for k in range(3):
            total = total + load_coded(lx.at[h, k], m // 16)
        return total

    store_coded(lysend, left_total(1 - yl))
    left_y = push(lysend, ly, flip_yl)
    lsum[...] = left_total(yl)

    a_y.wait_recv()
    next_a = slot(z, 1 - yh, 0)
    a_z += [push(next_a, next_a, z_peers[k - 1]) for k in (1, 2, 3)]

    g_d.wait_recv()
    core_all = jnp.concatenate([g0[pl.ds(0, r2), :], g0[pl.ds(r2, r2), :]], axis=1)
    gram = dot(core_all, core_all, ((0,), (0,)), HIGHEST)
    eye = jnp.where(
        lax.broadcasted_iota(jnp.int32, (r1, r1), 0) == lax.broadcasted_iota(jnp.int32, (r1, r1), 1), 1.0, 0.0
    )
    shift = jnp.sum(gram * eye, axis=(0, 1), keepdims=True) * 0.001 / r1
    gram = gram + shift * eye

    for k in (3, 1, 2):
        b_z[k - 1].wait_recv()
        from_z = slot((z + 4 - k) % 4, yh, 1)
        b_y.append(push(from_z, from_z, flip_yh))

    w = dot(core_all, inverse_256(gram), precision=HIGHEST)
    w_hi[...] = w.astype(BF16)
    w_lo[...] = (w - w_hi[...].astype(F32)).astype(BF16)

    left_y.wait_recv()
    left_out[...] = (lsum[...] + load_coded(ly, m // 16)).astype(BF16)

    for copy in a_z:
        copy.wait_recv()
    for copy in b_y:
        copy.wait_recv()

    @pl.loop(0, 8)
    def _(q):
        b = jnp.concatenate([load_coded(ag.at[q, 0], half), load_coded(ag.at[q, 1], half)], axis=0)
        hi = b.astype(BF16)
        lo = (b - hi.astype(F32)).astype(BF16)
        v = dot(hi, w_hi[...]) + (dot(hi, w_lo[...]) + dot(lo, w_hi[...]))
        right_out[pl.ds(pl.multiple_of(q * share, share), share), :] = v.astype(BF16)

    for copy in started:
        copy.wait_send()


def store(left_v, right_v, left_hbm, right_hbm, sem):
    copies = [
        pltpu.make_async_copy(right_v, right_hbm, sem.at[0]),
        pltpu.make_async_copy(left_v, left_hbm, sem.at[1]),
    ]
    for copy in copies:
        copy.start()
    for copy in copies:
        copy.wait()


def body(operator, right_test, left_test):
    m, n = operator.shape
    r1, r2 = right_test.shape[1], left_test.shape[1]
    left_rows, share = m // 16, n // 8
    coded = SCALE_ROWS
    vmem = pltpu.VMEM
    n1, n2 = r2 // 4, r2 // 16
    copies = 48
    outs = (
        jax.ShapeDtypeStruct((left_rows, r1), BF16),
        jax.ShapeDtypeStruct((n, r1), BF16),
    )
    left, right = pl.pallas_call(
        kernel,
        out_shape=outs,
        in_specs=[pl.BlockSpec(memory_space=pl.ANY)] * 3,
        out_specs=(pl.BlockSpec(memory_space=pltpu.VMEM),) * 2,
        scratch_shapes=[
            vmem((m, n), BF16), vmem((n, r1), BF16), vmem((m, r2), BF16), vmem((r2, m), BF16),
            vmem((4, r2, n // 4), F32), vmem((8, 2, left_rows, r1), F32),
            vmem((2 * r2, 128), F32), vmem((r2, 128), F32), vmem((r2, 128), F32),
            vmem((3, n1, 128), F32), vmem((n1, 128), F32), vmem((3, n2, 128), F32),
            vmem((n2, 128), F32), vmem((4, n2, 128), F32), vmem((2 * r2, 128), F32),
            vmem((3, 2, r2 + coded, share), BF16), vmem((3, 2, r2 + coded, share), BF16),
            vmem((r2, share), F32), vmem((r2 + coded, share), BF16), vmem((r2 + coded, share), BF16),
            vmem((8, 2, share // 2 + coded, r2), BF16),
            vmem((8, left_rows, r1), F32), vmem((2, 3, left_rows + coded, r1), BF16),
            vmem((2, 3, left_rows + coded, r1), BF16), vmem((left_rows, r1), F32),
            vmem((left_rows + coded, r1), BF16), vmem((left_rows + coded, r1), BF16),
            vmem((r2, r1), BF16), vmem((r2, r1), BF16),
            pltpu.SemaphoreType.DMA((9,)), pltpu.SemaphoreType.DMA((copies,)), pltpu.SemaphoreType.DMA((copies,)),
        ],
        compiler_params=pltpu.CompilerParams(
            collective_id=0, has_side_effects=True, vmem_limit_bytes=52 * 2**20
        ),
    )(operator, right_test, left_test)
    return pl.pallas_call(
        store,
        out_shape=outs,
        in_specs=[pl.BlockSpec(memory_space=pltpu.VMEM)] * 2,
        out_specs=(pl.BlockSpec(memory_space=pl.ANY),) * 2,
        scratch_shapes=[pltpu.SemaphoreType.DMA((2,))],
        compiler_params=pltpu.CompilerParams(vmem_limit_bytes=4 * 2**20),
    )(left, right)


def solution(mesh):
    placed = (P("row", "col"), P("col", None), P("row", None))
    return jax.shard_map(
        body,
        mesh=mesh,
        in_specs=placed,
        out_specs=(P(("row", "col"), None), P("col", None)),
        check_vma=False,
    )
```

```python
import jax
import jax.numpy as jnp
from jax import lax
from jax.experimental import pallas as pl
from jax.experimental.pallas import tpu as pltpu
from jax.sharding import PartitionSpec as P

MESH = pl.DeviceIdType.MESH
F32 = jnp.float32
BF16 = jnp.bfloat16
HIGHEST = lax.Precision.HIGHEST
SCALE_ROWS = 16
TOP = 2.0**15


def dot(a, b, dims=((1,), (0,)), precision=None):
    return lax.dot_general(a, b, (dims, ((), ())), precision=precision, preferred_element_type=F32)


def largest(value):
    return jnp.maximum(jnp.max(jnp.abs(value), axis=0, keepdims=True), 1e-30)


def store_coded(ref, value):
    rows, columns = value.shape
    scale = jnp.broadcast_to(largest(value) * 1.01, (SCALE_ROWS, columns)).astype(BF16)
    ref[pl.ds(rows, SCALE_ROWS), :] = scale
    t = value * (TOP / scale.astype(F32)[0:1, :])
    t2 = t * t
    t4 = t2 * t2
    t8 = t4 * t4
    ref[pl.ds(0, rows), :] = jnp.where(t < 0, -t8, t8).astype(BF16)


def load_coded(ref, rows):
    scale = ref[pl.ds(rows, SCALE_ROWS), :].astype(F32)[0:1, :] * (1.0 / TOP)
    y = ref[pl.ds(0, rows), :].astype(F32)
    r = jnp.exp2(jnp.log2(jnp.abs(y)) * 0.125) * scale
    return jnp.where(y < 0, -r, r)


def inverse_128(a):
    n = a.shape[0]
    sub = lax.broadcasted_iota(jnp.int32, (8, n), 0)
    lane8 = lax.broadcasted_iota(jnp.int32, (8, n), 1)
    lane = lax.broadcasted_iota(jnp.int32, (n, n), 1)
    for k0 in range(0, n, 8):
        p = a[k0 : k0 + 8, :]
        c = [jnp.broadcast_to(p[:, k0 + j : k0 + j + 1], (8, n)) for j in range(8)]
        for k in range(8):
            r = 1.0 / c[k][k : k + 1, :]
            ck = c[k]
            new = []
            for j in range(8):
                if j == k:
                    new.append(jnp.where(sub == k, r, -ck * r))
                else:
                    pj = c[j][k : k + 1, :] * r
                    new.append(jnp.where(sub == k, pj, c[j] - ck * pj))
            c = new
        inside8 = (lane8 >= k0) & (lane8 < k0 + 8)
        pivot = jnp.where(inside8, jnp.where(lane8 == sub + k0, 1.0, 0.0), p)
        x = c[0] * pivot[0:1, :]
        for j in range(1, 8):
            x = x + c[j] * pivot[j : j + 1, :]
        inside = (lane >= k0) & (lane < k0 + 8)
        rest = jnp.where(inside, 0.0, a)
        for j in range(8):
            rest = rest - a[:, k0 + j : k0 + j + 1] * x[j : j + 1, :]
        pieces = [rest[:k0]] * (k0 > 0) + [x] + [rest[k0 + 8 :]] * (k0 + 8 < n)
        a = jnp.concatenate(pieces, axis=0)
    return a


def inverse_256(g):
    h = g.shape[0] // 2
    a, b, d = g[:h, :h], g[:h, h:], g[h:, h:]
    ai = inverse_128(a)
    y = dot(ai, b, precision=HIGHEST)
    si = inverse_128(d - dot(b, y, ((0,), (0,)), HIGHEST))
    t = dot(y, si, precision=HIGHEST)
    top = ai + dot(t, y, ((1,), (1,)), HIGHEST)
    return jnp.concatenate(
        [jnp.concatenate([top, -t], axis=1), jnp.concatenate([-t.T, si], axis=1)], axis=0
    )


def kernel(
    a_hbm, r_hbm, l_hbm, left_out, right_out,
    a_v, r_v, l_v, lt_v, acc, lacc,
    cbuf, cd, h1, cx, h2, cy, h3, cz, g0,
    terms, far, relay, rsend, rz, rsum, ysend, ry, ag,
    ld, lsend, lx, lsum, lysend, ly, w_hi, w_lo,
    in_sem, ss, rs,
):
    m, n = a_hbm.shape
    r1 = r_hbm.shape[1]
    r2 = l_hbm.shape[1]
    row, col = lax.axis_index("row"), lax.axis_index("col")
    z, yh = row // 2, row % 2
    yl, x, core = col // 8, (col // 2) % 4, col % 2
    y = yh * 2 + yl
    share = n // 8
    group = 2 * share

    def dev(zz, yy, xx, cc):
        return (zz * 2 + yy // 2, (yy % 2) * 8 + xx * 2 + cc)

    chunk = m // 4
    load_l = []
    for i in range(4):
        part = pl.ds(i * chunk, chunk)
        load_l.append(pltpu.make_async_copy(l_hbm.at[part], l_v.at[part], in_sem.at[i]))
    order = (2, 1, 3, 0)
    columns = [pl.ds(pl.multiple_of(((z + k) % 4) * group, group), group) for k in order]
    load_a = [
        pltpu.make_async_copy(a_hbm.at[:, here], a_v.at[:, here], in_sem.at[4 + i])
        for i, here in enumerate(columns)
    ]
    load_r = pltpu.make_async_copy(r_hbm, r_v, in_sem.at[8])
    for load in load_l + load_a + [load_r]:
        load.start()

    partner = dev(z, y, x, 1 - core)
    z_peers = [dev((z + k) % 4, y, x, core) for k in (1, 2, 3)]
    y_peers = [dev(z, (y + k) % 4, x, core) for k in (1, 2, 3)]
    x_peers = [dev(z, y, (x + k) % 4, core) for k in (1, 2, 3)]
    xy_peers = [dev(z, yh * 2 + 1 - yl, (x + k) % 4, core) for k in (1, 2, 3)]
    flip_yl = dev(z, yh * 2 + 1 - yl, x, core)
    flip_yh = dev(z, (1 - yh) * 2 + yl, x, core)
    barrier = pltpu.get_barrier_semaphore()
    for peer in [partner] + z_peers + y_peers + x_peers + xy_peers:
        pl.semaphore_signal(barrier, inc=1, device_id=peer, device_id_type=MESH)

    count = [0]
    started = []

    def push(src, dst, peer):
        i = count[0]
        count[0] += 1
        copy = pltpu.make_async_remote_copy(
            src_ref=src, dst_ref=dst, send_sem=ss.at[i], recv_sem=rs.at[i],
            device_id=peer, device_id_type=MESH,
        )
        copy.start()
        started.append(copy)
        return copy

    for i in range(4):
        part = pl.ds(i * chunk, chunk)
        load_l[i].wait()
        lt_v[:, part] = l_v[part, :].T

    near = [[None, None], [None, None]]

    def send_far(h):
        store_coded(far.at[h], acc[0, :, h * share : (h + 1) * share])
        return push(far.at[h], relay.at[h], z_peers[2 * h])

    def send_near(side, h, value):
        store_coded(rsend.at[side, h], value)
        near[side][h] = push(rsend.at[side, h], rz.at[side, h], z_peers[2 * side])

    for i in range(4):
        load_a[i].wait()
        acc[i] = dot(lt_v[...], a_v[:, columns[i]])
        if i == 0:
            pl.semaphore_wait(barrier, 13)
            relayed = [send_far(0), send_far(1)]
        elif i == 1:
            send_near(0, 1, acc[1, :, share:])
        elif i == 2:
            send_near(1, 0, acc[2, :, :share])
        v = acc[i]
        hi = v.astype(BF16)
        v = v - hi.astype(F32)
        mid = v.astype(BF16)
        lo = (v - mid.astype(F32)).astype(BF16)
        terms[i, pl.ds(0, r2), :] = hi
        terms[i, pl.ds(r2, r2), :] = mid
        terms[i, pl.ds(2 * r2, r2), :] = lo

    load_r.wait()
    part = None
    for i in range(4):
        term = dot(terms[i], r_v[columns[i], :])
        part = term if part is None else part + term
    part = part[:r2] + (part[r2 : 2 * r2] + part[2 * r2 :])
    cbuf[pl.ds(0, r2), :] = part[:, :128]
    cbuf[pl.ds(r2, r2), :] = part[:, 128:]
    c_d = push(cbuf.at[pl.ds(pl.multiple_of((1 - core) * r2, 8), r2)], cd, partner)

    for copy in relayed:
        copy.wait_recv()
    send_near(0, 0, acc[1, :, :share] + load_coded(relay.at[0], r2))
    send_near(1, 1, acc[2, :, share:] + load_coded(relay.at[1], r2))

    def left_half(i):
        @pl.loop(0, 2)
        def _(t):
            rows = pl.ds(pl.multiple_of((2 * i + t) * (m // 4), m // 4), m // 4)
            product = dot(a_v[rows, :], r_v[...])
            lacc[pl.ds(4 * i + 2 * t, 2)] = product.reshape(2, 2, m // 16, r1)

        return push(lacc.at[pl.ds(4 * i, 4), 1 - core], ld.at[pl.ds(4 * i, 4)], partner)

    left_x = []

    def left_send(i):
        left_d[i].wait_recv()
        for k in (2, 1, 3):
            q = 4 * i + (x + k) % 4
            store_coded(lsend.at[i, k - 1], lacc[q, core] + ld[q])
            left_x.append(push(lsend.at[i, k - 1], lx.at[i, k - 1], x_peers[k - 1]))

    left_d = [left_half(0)]
    c_d.wait_recv()
    h1[...] = cbuf[pl.ds(pl.multiple_of(core * r2, 8), r2), :] + cd[...]
    n1 = r2 // 4
    c_x = [
        push(h1.at[pl.ds(pl.multiple_of(((x + k) % 4) * n1, 8), n1)], cx.at[k - 1], x_peers[k - 1])
        for k in (1, 2, 3)
    ]
    left_d.append(left_half(1))
    left_send(0)

    for copy in c_x:
        copy.wait_recv()
    h2[...] = h1[pl.ds(pl.multiple_of(x * n1, 8), n1), :] + (cx[0] + cx[1] + cx[2])
    n2 = n1 // 4
    c_y = [
        push(h2.at[pl.ds(pl.multiple_of(((y + k) % 4) * n2, 8), n2)], cy.at[k - 1], y_peers[k - 1])
        for k in (1, 2, 3)
    ]
    left_send(1)

    for copy in c_y:
        copy.wait_recv()
    h3[...] = h2[pl.ds(pl.multiple_of(y * n2, 8), n2), :] + (cy[0] + cy[1] + cy[2])
    cz[z] = h3[...]
    c_z = [push(h3, cz.at[z], z_peers[k - 1]) for k in (1, 2, 3)]

    for copy in near[0] + near[1]:
        copy.wait_recv()

    def right_total(h):
        here = pl.ds(pl.multiple_of(h * share, share), share)
        total = acc[3, :, here]
        for side in range(2):
            total = total + load_coded(rz.at[side, h], r2)
        return total

    store_coded(ysend, right_total(1 - yh))
    right_y = push(ysend, ry, flip_yh)
    rsum[...] = right_total(yh)

    for copy in c_z:
        copy.wait_recv()
    base2 = pl.multiple_of(core * r2 + x * n1, 8)
    base3 = pl.multiple_of(core * r2 + x * n1 + y * n2, 8)
    g0[pl.ds(base3, n2), :] = (cz[0] + cz[1]) + (cz[2] + cz[3])
    own = g0.at[pl.ds(base3, n2)]
    g_y = [push(own, own, y_peers[k - 1]) for k in (1, 2, 3)]

    for copy in g_y:
        copy.wait_recv()
    own = g0.at[pl.ds(base2, n1)]
    g_x = [push(own, own, x_peers[k - 1]) for k in (1, 2, 3)]

    right_y.wait_recv()
    v = (rsum[...] + load_coded(ry, r2)).T
    half = share // 2
    store_coded(ag.at[row, 1], v[half:])
    store_coded(ag.at[row, 0], v[:half])

    def slot(zz, yyh, which):
        return ag.at[zz * 2 + yyh, which]

    own_a, own_b = slot(z, yh, 0), slot(z, yh, 1)
    b_z = [push(own_b, own_b, z_peers[k - 1]) for k in (1, 2, 3)]
    a_y = push(own_a, own_a, flip_yh)
    b_y = [push(own_b, own_b, flip_yh)]
    a_z = [push(own_a, own_a, z_peers[k - 1]) for k in (1, 2, 3)]

    for copy in g_x:
        copy.wait_recv()
    own = g0.at[pl.ds(pl.multiple_of(core * r2, 8), r2)]
    g_d = push(own, own, partner)

    for copy in left_x:
        copy.wait_recv()

    def left_total(h):
        q = 4 * h + x
        total = lacc[q, core] + ld[q]
        for k in range(3):
            total = total + load_coded(lx.at[h, k], m // 16)
        return total

    store_coded(lysend, left_total(1 - yl))
    left_y = push(lysend, ly, flip_yl)
    lsum[...] = left_total(yl)

    a_y.wait_recv()
    next_a = slot(z, 1 - yh, 0)
    a_z += [push(next_a, next_a, z_peers[k - 1]) for k in (1, 2, 3)]

    g_d.wait_recv()
    core_all = jnp.concatenate([g0[pl.ds(0, r2), :], g0[pl.ds(r2, r2), :]], axis=1)
    gram = dot(core_all, core_all, ((0,), (0,)), HIGHEST)
    eye = jnp.where(
        lax.broadcasted_iota(jnp.int32, (r1, r1), 0) == lax.broadcasted_iota(jnp.int32, (r1, r1), 1), 1.0, 0.0
    )
    shift = jnp.sum(gram * eye, axis=(0, 1), keepdims=True) * 0.001 / r1
    gram = gram + shift * eye

    for k in (3, 1, 2):
        b_z[k - 1].wait_recv()
        from_z = slot((z + 4 - k) % 4, yh, 1)
        b_y.append(push(from_z, from_z, flip_yh))

    w = dot(core_all, inverse_256(gram), precision=HIGHEST)
    w_hi[...] = w.astype(BF16)
    w_lo[...] = (w - w_hi[...].astype(F32)).astype(BF16)

    left_y.wait_recv()
    left_out[...] = (lsum[...] + load_coded(ly, m // 16)).astype(BF16)

    for copy in a_z:
        copy.wait_recv()
    for copy in b_y:
        copy.wait_recv()

    @pl.loop(0, 8, unroll=2)
    def _(q):
        b = jnp.concatenate([load_coded(ag.at[q, 0], half), load_coded(ag.at[q, 1], half)], axis=0)
        hi = b.astype(BF16)
        lo = (b - hi.astype(F32)).astype(BF16)
        v = dot(hi, w_hi[...]) + (dot(hi, w_lo[...]) + dot(lo, w_hi[...]))
        right_out[pl.ds(pl.multiple_of(q * share, share), share), :] = v.astype(BF16)

    for copy in started:
        copy.wait_send()


def store(left_v, right_v, left_hbm, right_hbm, sem):
    copies = [
        pltpu.make_async_copy(right_v, right_hbm, sem.at[0]),
        pltpu.make_async_copy(left_v, left_hbm, sem.at[1]),
    ]
    for copy in copies:
        copy.start()
    for copy in copies:
        copy.wait()


def body(operator, right_test, left_test):
    m, n = operator.shape
    r1, r2 = right_test.shape[1], left_test.shape[1]
    left_rows, share = m // 16, n // 8
    coded = SCALE_ROWS
    vmem = pltpu.VMEM
    n1, n2 = r2 // 4, r2 // 16
    copies = 48
    outs = (
        jax.ShapeDtypeStruct((left_rows, r1), BF16),
        jax.ShapeDtypeStruct((n, r1), BF16),
    )
    left, right = pl.pallas_call(
        kernel,
        out_shape=outs,
        in_specs=[pl.BlockSpec(memory_space=pl.ANY)] * 3,
        out_specs=(pl.BlockSpec(memory_space=pltpu.VMEM),) * 2,
        scratch_shapes=[
            vmem((m, n), BF16), vmem((n, r1), BF16), vmem((m, r2), BF16), vmem((r2, m), BF16),
            vmem((4, r2, n // 4), F32), vmem((8, 2, left_rows, r1), F32),
            vmem((2 * r2, 128), F32), vmem((r2, 128), F32), vmem((r2, 128), F32),
            vmem((3, n1, 128), F32), vmem((n1, 128), F32), vmem((3, n2, 128), F32),
            vmem((n2, 128), F32), vmem((4, n2, 128), F32), vmem((2 * r2, 128), F32),
            vmem((4, 3 * r2, n // 4), BF16), vmem((2, r2 + coded, share), BF16), vmem((2, r2 + coded, share), BF16),
            vmem((2, 2, r2 + coded, share), BF16), vmem((2, 2, r2 + coded, share), BF16),
            vmem((r2, share), F32), vmem((r2 + coded, share), BF16), vmem((r2 + coded, share), BF16),
            vmem((8, 2, share // 2 + coded, r2), BF16),
            vmem((8, left_rows, r1), F32), vmem((2, 3, left_rows + coded, r1), BF16),
            vmem((2, 3, left_rows + coded, r1), BF16), vmem((left_rows, r1), F32),
            vmem((left_rows + coded, r1), BF16), vmem((left_rows + coded, r1), BF16),
            vmem((r2, r1), BF16), vmem((r2, r1), BF16),
            pltpu.SemaphoreType.DMA((9,)), pltpu.SemaphoreType.DMA((copies,)), pltpu.SemaphoreType.DMA((copies,)),
        ],
        compiler_params=pltpu.CompilerParams(
            collective_id=0, has_side_effects=True, vmem_limit_bytes=52 * 2**20
        ),
    )(operator, right_test, left_test)
    return pl.pallas_call(
        store,
        out_shape=outs,
        in_specs=[pl.BlockSpec(memory_space=pltpu.VMEM)] * 2,
        out_specs=(pl.BlockSpec(memory_space=pl.ANY),) * 2,
        scratch_shapes=[pltpu.SemaphoreType.DMA((2,))],
        compiler_params=pltpu.CompilerParams(vmem_limit_bytes=4 * 2**20),
    )(left, right)


def solution(mesh):
    placed = (P("row", "col"), P("col", None), P("row", None))
    return jax.shard_map(
        body,
        mesh=mesh,
        in_specs=placed,
        out_specs=(P(("row", "col"), None), P("col", None)),
        check_vma=False,
    )
```
